8 devices in a mesh: data: 8 (over z, y, x, core).
Axes of the slice: x: 2, y: 2, z: 1, core: 2. Of those that a mesh axis runs over, the one named last changes fastest.
Arguments:
- z_one: bfloat16 [512, 256], P('data')
- z_two: bfloat16 [512, 256], P('data')
- protos: bfloat16 [8192, 256], replicated
- queue_one: bfloat16 [2048, 256], P('data')
- queue_two: bfloat16 [2048, 256], P('data')
Outputs:
- output 1: float32 [512, 8192], P('data')
- output 2: float32 [512, 8192], P('data')
- output 3: float32 [], replicated
- output 4: float32 [512, 256], P('data')
- output 5: float32 [512, 256], P('data')
- output 6: float32 [8192, 256], replicated
All inputs are finite; a program needn't handle non-finite values.
Results may differ from the reference program's by a relative error of at most 0.001.
Values are sent between devices in bfloat16 or wider.
A program may use at most 1 GiB of HBM per device.

```python
import jax
import jax.numpy as jnp
from jax import lax

PROTOS = 8192
EMBED_DIM = 256
GROUP_SIZE = 8
ROWS_DEV = 64
QUEUE_DEV = 256
SINKHORN_ITERS = 3
EPSILON = 0.05
TEMPERATURE = 0.1


def unit_rows(values):
    return values / jnp.sqrt(jnp.sum(values * values, axis=-1, keepdims=True))


def setup_inputs(seed: int = 0) -> dict:
    key_list = jax.random.split(jax.random.key(seed), 8)
    noise_scale = EMBED_DIM ** -0.5
    batch_shape = (GROUP_SIZE, ROWS_DEV, EMBED_DIM)
    queue_shape = (GROUP_SIZE, QUEUE_DEV, EMBED_DIM)
    centers = unit_rows(jax.random.normal(key_list[0], (GROUP_SIZE, 1, EMBED_DIM), jnp.float32))
    queue_centers = unit_rows(jax.random.normal(key_list[1], (GROUP_SIZE, 1, EMBED_DIM), jnp.float32))
    base_rows = 1.5 * centers + noise_scale * jax.random.normal(key_list[2], batch_shape, jnp.float32)
    view_one = unit_rows(base_rows + 0.5 * noise_scale * jax.random.normal(key_list[3], batch_shape, jnp.float32))
    view_two = unit_rows(base_rows + 0.5 * noise_scale * jax.random.normal(key_list[4], batch_shape, jnp.float32))
    queue_one = unit_rows(1.5 * queue_centers + noise_scale * jax.random.normal(key_list[5], queue_shape, jnp.float32))
    queue_two = unit_rows(1.5 * queue_centers + noise_scale * jax.random.normal(key_list[6], queue_shape, jnp.float32))
    protos = unit_rows(jax.random.normal(key_list[7], (PROTOS, EMBED_DIM), jnp.float32))
    return {
        "z_one": view_one.reshape(GROUP_SIZE * ROWS_DEV, EMBED_DIM).astype(jnp.bfloat16),
        "z_two": view_two.reshape(GROUP_SIZE * ROWS_DEV, EMBED_DIM).astype(jnp.bfloat16),
        "protos": protos.astype(jnp.bfloat16),
        "queue_one": queue_one.reshape(GROUP_SIZE * QUEUE_DEV, EMBED_DIM).astype(jnp.bfloat16),
        "queue_two": queue_two.reshape(GROUP_SIZE * QUEUE_DEV, EMBED_DIM).astype(jnp.bfloat16),
    }


def scores_of(row_block, protos):
    return jnp.dot(row_block, protos.T, preferred_element_type=jnp.float32)


def scaled_col_sum(blocks, protos, col_scale, total_rows):
    def pass_body(col_acc, row_block):
        transport = jnp.exp(scores_of(row_block, protos) / EPSILON)
        row_scale = 1.0 / (total_rows * jnp.sum(transport * col_scale, axis=1))
        return col_acc + jnp.sum(transport * row_scale[:, None], axis=0), None
    col_sum, _ = lax.scan(pass_body, jnp.zeros((PROTOS,), jnp.float32), blocks)
    return col_sum


def column_scale(blocks, protos):
    total_rows = GROUP_SIZE * (ROWS_DEV + QUEUE_DEV)

    def first_body(col_acc, row_block):
        transport = jnp.exp(scores_of(row_block, protos) / EPSILON)
        return col_acc + jnp.sum(transport, axis=0), None

    col_sum, _ = lax.scan(first_body, jnp.zeros((PROTOS,), jnp.float32), blocks)
    col_scale = 1.0 / (PROTOS * col_sum)
    for _ in range(SINKHORN_ITERS - 1):
        col_scale = 1.0 / (PROTOS * scaled_col_sum(blocks, protos, col_scale, total_rows))
    return col_scale


def reference(z_one, z_two, protos, queue_one, queue_two):
    batch_one = z_one.reshape(GROUP_SIZE, ROWS_DEV, EMBED_DIM)
    batch_two = z_two.reshape(GROUP_SIZE, ROWS_DEV, EMBED_DIM)
    rows_all_one = jnp.concatenate([batch_one, queue_one.reshape(GROUP_SIZE, QUEUE_DEV, EMBED_DIM)], axis=1)
    rows_all_two = jnp.concatenate([batch_two, queue_two.reshape(GROUP_SIZE, QUEUE_DEV, EMBED_DIM)], axis=1)
    scale_one = column_scale(rows_all_one, protos)
    scale_two = column_scale(rows_all_two, protos)
    batch_total = GROUP_SIZE * ROWS_DEV
    grad_coef = 1.0 / (2 * batch_total * TEMPERATURE)

    def block_step(carry, row_blocks):
        loss_acc, proto_acc = carry
        rows_one, rows_two = row_blocks
        score_one = scores_of(rows_one, protos)
        score_two = scores_of(rows_two, protos)
        plan_one = jnp.exp(score_one / EPSILON) * scale_one
        plan_two = jnp.exp(score_two / EPSILON) * scale_two
        codes_one = plan_one / jnp.sum(plan_one, axis=1, keepdims=True)
        codes_two = plan_two / jnp.sum(plan_two, axis=1, keepdims=True)
        logp_one = jax.nn.log_softmax(score_one / TEMPERATURE, axis=1)
        logp_two = jax.nn.log_softmax(score_two / TEMPERATURE, axis=1)
        part_loss = jnp.sum(codes_two * logp_one) + jnp.sum(codes_one * logp_two)
        grad_s_one = ((jnp.exp(logp_one) - codes_two) * grad_coef).astype(jnp.bfloat16)
        grad_s_two = ((jnp.exp(logp_two) - codes_one) * grad_coef).astype(jnp.bfloat16)
        dz_one = jnp.dot(grad_s_one, protos, preferred_element_type=jnp.float32)
        dz_two = jnp.dot(grad_s_two, protos, preferred_element_type=jnp.float32)
        proto_part = jnp.dot(grad_s_one.T, rows_one, preferred_element_type=jnp.float32) + jnp.dot(grad_s_two.T, rows_two, preferred_element_type=jnp.float32)
        return (loss_acc + part_loss, proto_acc + proto_part), (codes_one, codes_two, dz_one, dz_two)

    start_carry = (jnp.zeros((), jnp.float32), jnp.zeros((PROTOS, EMBED_DIM), jnp.float32))
    (loss_sum, grad_protos), (codes_one, codes_two, dz_one, dz_two) = lax.scan(block_step, start_carry, (batch_one, batch_two))
    swap_loss = -loss_sum / (2 * batch_total)
    return (
        codes_one.reshape(batch_total, PROTOS),
        codes_two.reshape(batch_total, PROTOS),
        swap_loss,
        dz_one.reshape(batch_total, EMBED_DIM),
        dz_two.reshape(batch_total, EMBED_DIM),
        grad_protos,
    )
```

```python
import functools
import math

import jax
import jax.numpy as jnp
from jax import lax
from jax.experimental import pallas as pl
from jax.experimental.pallas import tpu as pltpu
from jax.sharding import PartitionSpec as P

MESH = pl.DeviceIdType.MESH
F32 = jnp.float32
BF16 = jnp.bfloat16
LOG2E = math.log2(math.e)
K20 = 20.0 * LOG2E
K10 = 10.0 * LOG2E
ITERS = 3
NB = 64
NQ = 256
NR = NB + NQ
D = 256
K = 8192
H = K // 2
TOTAL = 8 * NR
T = 512
NT = (((1,), (1,)), ((), ()))
NN = (((1,), (0,)), ((), ()))


def iota(shape, dim):
    return lax.broadcasted_iota(jnp.int32, shape, dim)


def sink_kernel(z1, z2, q1, q2, protos, za, c_out, nrm,
                ch, qp, xb, e, sb, cb, rb, arb, rsb, fb,
                load_sem, zs, zr, xs, xr, fs, fr, cs, cr, as_, ar, rs_, rr, ns, nr, ds_, dr):
    me = lax.axis_index("data")
    core = lax.rem(me, 2)
    chip = me // 2
    px = chip + 1 - 2 * lax.rem(chip, 2)
    py = lax.rem(chip + 2, 4)
    pd = 3 - chip
    peers = [px * 2 + core, py * 2 + core, pd * 2 + core]
    peer_chips = [px, py, pd]
    mate = me + 1 - 2 * core
    other = 1 - core

    loads = []
    for t in range(4):
        loads.append(pltpu.make_async_copy(
            protos.at[pl.ds(core * H + t * 1024, 1024)], ch.at[pl.ds(t * 1024, 1024)], load_sem.at[t]))
        loads[-1].start()

    bar = pltpu.get_barrier_semaphore()
    for dev in peers + [mate]:
        pl.semaphore_signal(bar, inc=1, device_id=(dev,), device_id_type=MESH)
    pl.semaphore_wait(bar, 4)

    def remote(src, dst, ssem, rsem, dev):
        return pltpu.make_async_remote_copy(src_ref=src, dst_ref=dst, send_sem=ssem, recv_sem=rsem,
                                            device_id=(dev,), device_id_type=MESH)

    zrows = pl.ds(pl.multiple_of(me * NB, NB), NB)
    sends = []
    zin = [z1, z2]
    qin = [q1, q2]
    for v in range(2):
        cp = remote(zin[v], za.at[v, zrows], xs.at[v], xr.at[v], mate)
        cp.start()
        sends.append(cp)
    for v in range(2):
        cp = remote(qin[v], qp.at[v], xs.at[2 + v], xr.at[2 + v], mate)
        cp.start()
        sends.append(cp)
    zcopies = []
    for p in range(3):
        for v in range(2):
            cp = remote(zin[v], za.at[v, zrows], zs.at[p, v], zr.at[p, v], peers[p])
            cp.start()
            zcopies.append(cp)

    for v in range(2):
        za[v, zrows, :] = zin[v][...]
        xb[core, v, 0:NB, :] = zin[v][...]
        xb[core, v, NB:NR, :] = qin[v][...]

    def score_block(c, first):
        def body(t, carry):
            cols = pl.ds(pl.multiple_of(t * T, T), T)
            ct = ch[cols, :]
            for v in range(2):
                s = lax.dot_general(xb[c, v], ct, NT, preferred_element_type=F32)
                ex = jnp.exp2(s * K20)
                e[v, pl.ds(pl.multiple_of(c * NR, NB), NR), cols] = ex
                sb[v, pl.ds(pl.multiple_of(c * NB, NB), NB), cols] = s[0:NB]
                col = jnp.sum(ex, axis=0, keepdims=True)
                if first:
                    arb[0, v, chip, :, cols] = col
                else:
                    arb[0, v, chip, :, cols] = arb[0, v, chip, :, cols] + col
            return carry
        return body

    per = H // T // 4
    for t in range(4):
        loads[t].wait()
        lax.fori_loop(t * per, (t + 1) * per, score_block(core, True), 0)

    for cp in sends:
        cp.wait_recv()
    mrows = pl.ds(pl.multiple_of(mate * NB, NB), NB)
    for v in range(2):
        xb[other, v, 0:NB, :] = za[v, mrows, :]
        xb[other, v, NB:NR, :] = qp[v]
    lax.fori_loop(0, H // T, score_block(other, False), 0)

    def send_cols(it, v):
        out = []
        for p in range(3):
            cp = remote(arb.at[it, v, chip], arb.at[it, v, chip], as_.at[it, v, p], ar.at[it, v, p], peers[p])
            cp.start()
            out.append(cp)
        return out

    flight = [send_cols(0, v) for v in range(2)]

    for cp in zcopies:
        cp.wait_recv()
    fwd = []
    for p in range(3):
        rows = pl.ds(pl.multiple_of(peers[p] * NB, NB), NB)
        for v in range(2):
            cp = remote(za.at[v, rows], za.at[v, rows], fs.at[p, v], fr.at[p, v], mate)
            cp.start()
            fwd.append(cp)

    ccopies = []

    def scale(it, v):
        for cp in flight[v]:
            cp.wait_recv()
        tot = (arb[it, v, 0] + arb[it, v, 1]) + (arb[it, v, 2] + arb[it, v, 3])
        cval = 1.0 / (K * tot)
        cb[v] = jnp.broadcast_to(cval, (8, H))
        if it == ITERS - 1:
            c_out[v, core] = cval
            cp = remote(c_out.at[v, core], c_out.at[v, core], cs.at[v], cr.at[v], mate)
            cp.start()
            ccopies.append(cp)

    lane8 = iota((8, 128), 1)
    sub8 = iota((8, 128), 0)

    def row_pass(it, v):
        def body(i, pack):
            accs = [jnp.zeros((8, 128), F32)] * 8
            for k in range(H // 128):
                ck = cb[v, :, k * 128:(k + 1) * 128]
                for g in range(8):
                    r0 = pl.multiple_of(i * 64 + g * 8, 8)
                    accs[g] = accs[g] + e[v, pl.ds(r0, 8), k * 128:(k + 1) * 128] * ck
            for g in range(8):
                rs = jnp.sum(accs[g], axis=1, keepdims=True)
                pack = jnp.where(lane8 == i * 8 + g, rs, pack)
            return pack
        pack = lax.fori_loop(0, 2 * NR // 64, body, jnp.zeros((8, 128), F32))
        rsb[it, v, core] = pack
        cp = remote(rsb.at[it, v, core], rsb.at[it, v, core], rs_.at[it, v], rr.at[it, v], mate)
        cp.start()
        return cp

    def col_pass(it, v, cp):
        cp.wait_recv()
        rtot = rsb[it, v, 0] + rsb[it, v, 1]
        r = 1.0 / (TOTAL * rtot)
        for g in range(2 * NR // 8):
            rb[v, g * 8:(g + 1) * 8, :] = jnp.broadcast_to(r[:, g:g + 1], (8, 128))
        for cc in range(4):
            def body(i, accs):
                accs = list(accs)
                for g in range(8):
                    r0 = pl.multiple_of(i * 64 + g * 8, 8)
                    rg = rb[v, pl.ds(r0, 8), :]
                    for k in range(8):
                        lo = cc * 1024 + k * 128
                        accs[k] = accs[k] + e[v, pl.ds(r0, 8), lo:lo + 128] * rg
                return tuple(accs)
            accs = lax.fori_loop(0, 2 * NR // 64, body, tuple(jnp.zeros((8, 128), F32) for _ in range(8)))
            for k in range(8):
                lo = cc * 1024 + k * 128
                arb[it + 1, v, chip, :, lo:lo + 128] = jnp.sum(accs[k], axis=0, keepdims=True)

    drain = []
    rcopies = []
    for it in range(ITERS - 1):
        cps = []
        for v in range(2):
            scale(it, v)
            cps.append(row_pass(it, v))
        drain += flight[0] + flight[1]
        rcopies += cps
        flight = [None, None]
        for v in range(2):
            col_pass(it, v, cps[v])
            flight[v] = send_cols(it + 1, v)

    def to_row(total, gg, col):
        return total + jnp.where(lane8 == gg * 8 + sub8, col, 0.0)

    def p_pass(v):
        def body(i, total):
            accs = [jnp.zeros((8, 128), F32)] * 8
            for k in range(H // 128):
                for g in range(8):
                    r0 = pl.multiple_of(i * 64 + g * 8, 8)
                    accs[g] = accs[g] + jnp.exp2(sb[v, pl.ds(r0, 8), k * 128:(k + 1) * 128] * K10)
            for g in range(8):
                total = to_row(total, i * 8 + g, jnp.sum(accs[g], axis=1, keepdims=True))
            return total
        total = lax.fori_loop(0, 2, body, jnp.zeros((8, 128), F32))
        fb[core, 4 + v:5 + v, :] = jnp.sum(total, axis=0, keepdims=True)

    def last_pass(v):
        def body(i, totals):
            tr, tl = totals
            for half in range(2):
                ra = [jnp.zeros((8, 128), F32)] * 4
                la = [jnp.zeros((8, 128), F32)] * 4
                for k in range(H // 128):
                    ck = cb[v, :, k * 128:(k + 1) * 128]
                    for g in range(4):
                        off = half * 32 + g * 8
                        re = pl.multiple_of(i * NR + off, 8)
                        rb_ = pl.multiple_of(i * NB + off, 8)
                        ec = e[v, pl.ds(re, 8), k * 128:(k + 1) * 128] * ck
                        ra[g] = ra[g] + ec
                        la[g] = la[g] + ec * sb[1 - v, pl.ds(rb_, 8), k * 128:(k + 1) * 128]
                for g in range(4):
                    gg = i * 8 + half * 4 + g
                    tr = to_row(tr, gg, jnp.sum(ra[g], axis=1, keepdims=True))
                    tl = to_row(tl, gg, jnp.sum(la[g], axis=1, keepdims=True))
            return tr, tl
        zero = jnp.zeros((8, 128), F32)
        tr, tl = lax.fori_loop(0, 2, body, (zero, zero))
        fb[core, v:v + 1, :] = jnp.sum(tr, axis=0, keepdims=True)
        fb[core, 2 + v:3 + v, :] = jnp.sum(tl, axis=0, keepdims=True)

    fb[core, 6:8, :] = jnp.zeros((2, 128), F32)
    for v in range(2):
        p_pass(v)
    for v in range(2):
        scale(ITERS - 1, v)
        last_pass(v)
    drain += flight[0] + flight[1]
    cp = remote(fb.at[core], fb.at[core], ds_, dr, mate)
    cp.start()
    cp.wait_recv()
    tot = fb[0] + fb[1]
    rinv = 1.0 / tot[0:2]
    pinv = 1.0 / tot[4:6]
    logp = jnp.log(tot[4:6])
    mean = tot[2:4] * rinv * 10.0
    loss = jnp.sum(mean - logp, axis=0, keepdims=True)
    nrm[chip, 0:2, :] = rinv
    nrm[chip, 2:4, :] = pinv
    nrm[chip, 4:5, :] = loss
    nrm[chip, 5:8, :] = jnp.zeros((3, 128), F32)
    ncopies = []
    for p in range(3):
        n = remote(nrm.at[chip], nrm.at[chip], ns.at[p], nr.at[p], peers[p])
        n.start()
        ncopies.append(n)
    cp.wait_send()
    for c in sends + zcopies + drain + rcopies:
        c.wait_send()
    for c in fwd + ccopies + ncopies:
        c.wait()


def sink_call(z1, z2, q1, q2, protos):
    vmem = pl.BlockSpec(memory_space=pltpu.VMEM)
    dma = pltpu.SemaphoreType.DMA
    return pl.pallas_call(
        sink_kernel,
        out_shape=(
            jax.ShapeDtypeStruct((2, 8 * NB, D), BF16),
            jax.ShapeDtypeStruct((2, 2, 1, H), F32),
            jax.ShapeDtypeStruct((4, 8, 128), F32),
        ),
        in_specs=[vmem] * 4 + [pl.BlockSpec(memory_space=pl.ANY)],
        out_specs=(vmem, vmem, vmem),
        scratch_shapes=[
            pltpu.VMEM((H, D), BF16),
            pltpu.VMEM((2, NQ, D), BF16),
            pltpu.VMEM((2, 2, NR, D), BF16),
            pltpu.VMEM((2, 2 * NR, H), F32),
            pltpu.VMEM((2, 2 * NB, H), F32),
            pltpu.VMEM((2, 8, H), F32),
            pltpu.VMEM((2, 2 * NR, 128), F32),
            pltpu.VMEM((ITERS, 2, 4, 1, H), F32),
            pltpu.VMEM((ITERS - 1, 2, 2, 8, 128), F32),
            pltpu.VMEM((2, 8, 128), F32),
            dma((4,)),
            dma((3, 2)), dma((3, 2)),
            dma((4,)), dma((4,)),
            dma((3, 2)), dma((3, 2)),
            dma((2,)), dma((2,)),
            dma((ITERS, 2, 3)), dma((ITERS, 2, 3)),
            dma((ITERS - 1, 2)), dma((ITERS - 1, 2)),
            dma((3,)), dma((3,)),
            dma, dma,
        ],
        compiler_params=pltpu.CompilerParams(collective_id=0, has_side_effects=True,
                                             vmem_limit_bytes=60 * 1024 * 1024),
        name="sink",
    )(z1, z2, q1, q2, protos)


TK = 512
COEF = 1.0 / (1024 * 0.1)


def grad_kernel(z1, z2, za, protos, c, nrm, codes1, codes2, dz1, dz2, gp, loss, own, prow):
    step = pl.program_id(0)

    @pl.when(step == 0)
    def _():
        me = lax.axis_index("data")
        core = lax.rem(me, 2)
        chip = me // 2
        mine = nrm[chip]
        pick = iota((NB, 128), 1) == iota((NB, 128), 0) + core * NB
        for q in range(4):
            col = jnp.sum(jnp.where(pick, jnp.broadcast_to(mine[q:q + 1], (NB, 128)), 0.0), axis=1, keepdims=True)
            own[q] = jnp.broadcast_to(col, (NB, 128))
            for d in range(4):
                prow[q, :, d * 128:(d + 1) * 128] = nrm[d, q:q + 1, :] * COEF
        tot = jnp.zeros((1, 128), F32)
        for d in range(4):
            tot = tot + nrm[d, 4:5, :]
        loss[...] = jnp.sum(tot, axis=1, keepdims=True) * (-1.0 / 1024)
        dz1[...] = jnp.zeros_like(dz1)
        dz2[...] = jnp.zeros_like(dz2)

    ct = protos[...]
    crow = [c[v] for v in range(2)]

    ex = []
    for z in (z1, z2):
        s = lax.dot_general(z[...], ct, NT, preferred_element_type=F32)
        ex.append(jnp.exp2(s * K10))
    code = []
    for v, out in enumerate((codes1, codes2)):
        q = ex[v] * ex[v] * crow[v] * own[v, :, 0:1]
        out[...] = q
        code.append(q)
    for v, dz in enumerate((dz1, dz2)):
        g = ((ex[v] * own[2 + v, :, 0:1] - code[1 - v]) * COEF).astype(BF16)
        dz[...] += lax.dot_general(g, ct, NN, preferred_element_type=F32)

    for b in range(TK // 128):
        rows = slice(b * 128, (b + 1) * 128)
        cb = ct[rows]
        et = []
        for v in range(2):
            s = lax.dot_general(cb, za[v], NT, preferred_element_type=F32)
            et.append(jnp.exp2(s * K10))
        acc = None
        for v in range(2):
            ccol = jnp.broadcast_to(crow[1 - v][:, b * 128:(b + 1) * 128], (128, 128)).T
            ccol = jnp.concatenate([ccol] * 4, axis=1)
            g = et[v] * prow[2 + v] - et[1 - v] * et[1 - v] * (ccol * prow[1 - v])
            part = lax.dot_general(g.astype(BF16), za[v], NN, preferred_element_type=F32)
            acc = part if acc is None else acc + part
        gp[rows, :] = acc


def grad_call(z1, z2, za, protos, c, nrm):
    full = lambda *shape: pl.BlockSpec(shape, lambda t: (0,) * len(shape))
    return pl.pallas_call(
        grad_kernel,
        grid=(K // TK,),
        out_shape=(
            jax.ShapeDtypeStruct((NB, K), F32),
            jax.ShapeDtypeStruct((NB, K), F32),
            jax.ShapeDtypeStruct((NB, D), F32),
            jax.ShapeDtypeStruct((NB, D), F32),
            jax.ShapeDtypeStruct((K, D), F32),
            jax.ShapeDtypeStruct((1, 1), F32),
        ),
        in_specs=[
            full(NB, D), full(NB, D), full(2, 8 * NB, D),
            pl.BlockSpec((TK, D), lambda t: (t, 0)),
            pl.BlockSpec((2, 1, TK), lambda t: (0, 0, t)),
            full(4, 8, 128),
        ],
        out_specs=(
            pl.BlockSpec((NB, TK), lambda t: (0, t)),
            pl.BlockSpec((NB, TK), lambda t: (0, t)),
            full(NB, D), full(NB, D),
            pl.BlockSpec((TK, D), lambda t: (t, 0)),
            full(1, 1),
        ),
        scratch_shapes=[pltpu.VMEM((4, NB, 128), F32), pltpu.VMEM((4, 1, 8 * NB), F32)],
        compiler_params=pltpu.CompilerParams(dimension_semantics=("arbitrary",)),
        name="grads",
    )(z1, z2, za, protos, c, nrm)


def solution(mesh):
    def local_step(z1, z2, protos, q1, q2):
        za, c, nrm = sink_call(z1, z2, q1, q2, protos)
        c = c.reshape(2, 1, K)
        codes1, codes2, dz1, dz2, gp, loss = grad_call(z1, z2, za, protos, c, nrm)
        return codes1, codes2, loss.reshape(()), dz1, dz2, gp

    row = P("data", None)
    full = P(None, None)
    return jax.shard_map(
        local_step,
        mesh=mesh,
        in_specs=(row, row, full, row, row),
        out_specs=(row, row, P(), row, row, full),
        check_vma=False,
    )
```

```python
import functools
import math

import jax
import jax.numpy as jnp
from jax import lax
from jax.experimental import pallas as pl
from jax.experimental.pallas import tpu as pltpu
from jax.sharding import PartitionSpec as P

MESH = pl.DeviceIdType.MESH
F32 = jnp.float32
BF16 = jnp.bfloat16
LOG2E = math.log2(math.e)
K20 = 20.0 * LOG2E
K10 = 10.0 * LOG2E
ITERS = 3
NB = 64
NQ = 256
NR = NB + NQ
D = 256
K = 8192
H = K // 2
TOTAL = 8 * NR
T = 1024
NT = (((1,), (1,)), ((), ()))
NN = (((1,), (0,)), ((), ()))


def iota(shape, dim):
    return lax.broadcasted_iota(jnp.int32, shape, dim)


def sink_kernel(z1, z2, q1, q2, protos, za, c_out, nrm,
                ch, xb, e, sb, cb, rb, arb, rsb, fb,
                in_sem, load_sem, zs, zr, xs, xr, fs, fr, cs, cr, as_, ar, rs_, rr, ns, nr, ds_, dr):
    me = lax.axis_index("data")
    core = lax.rem(me, 2)
    chip = me // 2
    px = chip + 1 - 2 * lax.rem(chip, 2)
    py = lax.rem(chip + 2, 4)
    pd = 3 - chip
    peers = [px * 2 + core, py * 2 + core, pd * 2 + core]
    peer_chips = [px, py, pd]
    mate = me + 1 - 2 * core
    other = 1 - core

    zrows = pl.ds(pl.multiple_of(me * NB, NB), NB)
    rows_in = []
    for v, (z, q) in enumerate(((z1, q1), (z2, q2))):
        rows_in.append(pltpu.make_async_copy(z, xb.at[core, v, pl.ds(0, NB)], in_sem.at[v, 0]))
        rows_in.append(pltpu.make_async_copy(q, xb.at[core, v, pl.ds(NB, NQ)], in_sem.at[v, 1]))
        rows_in.append(pltpu.make_async_copy(z, za.at[v, zrows], in_sem.at[v, 2]))
    for cp in rows_in:
        cp.start()
    loads = []
    for t in range(4):
        loads.append(pltpu.make_async_copy(
            protos.at[pl.ds(core * H + t * 1024, 1024)], ch.at[pl.ds(t * 1024, 1024)], load_sem.at[t]))
        loads[-1].start()

    bar = pltpu.get_barrier_semaphore()
    for dev in peers + [mate]:
        pl.semaphore_signal(bar, inc=1, device_id=(dev,), device_id_type=MESH)

    def remote(src, dst, ssem, rsem, dev):
        return pltpu.make_async_remote_copy(src_ref=src, dst_ref=dst, send_sem=ssem, recv_sem=rsem,
                                            device_id=(dev,), device_id_type=MESH)

    def score_block(c, first):
        def body(t, carry):
            cols = pl.ds(pl.multiple_of(t * T, T), T)
            ct = ch[cols, :]
            for v in range(2):
                s = lax.dot_general(xb[c, v], ct, NT, preferred_element_type=F32)
                ex = jnp.exp2(s * K20)
                e[v, pl.ds(pl.multiple_of(c * NR, NB), NR), cols] = ex
                sb[v, pl.ds(pl.multiple_of(c * NB, NB), NB), cols] = s[0:NB]
                col = jnp.sum(ex, axis=0, keepdims=True)
                if first:
                    arb[0, v, chip, :, cols] = col
                else:
                    arb[0, v, chip, :, cols] = arb[0, v, chip, :, cols] + col
            return carry
        return body

    for cp in rows_in:
        cp.wait()
    loads[0].wait()
    score_block(core, True)(0, 0)
    pl.semaphore_wait(bar, 4)
    sends = []
    for v in range(2):
        cp = remote(xb.at[core, v], xb.at[core, v], xs.at[v], xr.at[v], mate)
        cp.start()
        sends.append(cp)
        cp = remote(za.at[v, zrows], za.at[v, zrows], xs.at[2 + v], xr.at[2 + v], mate)
        cp.start()
        sends.append(cp)
    zcopies = []
    for p in range(3):
        for v in range(2):
            cp = remote(za.at[v, zrows], za.at[v, zrows], zs.at[p, v], zr.at[p, v], peers[p])
            cp.start()
            zcopies.append(cp)
    for t in range(1, 4):
        loads[t].wait()
    lax.fori_loop(1, H // T, score_block(core, True), 0)

    for cp in sends:
        cp.wait_recv()
    lax.fori_loop(0, H // T, score_block(other, False), 0)

    def send_cols(it, v):
        out = []
        for p in range(3):
            cp = remote(arb.at[it, v, chip], arb.at[it, v, chip], as_.at[it, v, p], ar.at[it, v, p], peers[p])
            cp.start()
            out.append(cp)
        return out

    flight = [send_cols(0, v) for v in range(2)]

    for cp in zcopies:
        cp.wait_recv()
    fwd = []
    for p in range(3):
        rows = pl.ds(pl.multiple_of(peers[p] * NB, NB), NB)
        for v in range(2):
            cp = remote(za.at[v, rows], za.at[v, rows], fs.at[p, v], fr.at[p, v], mate)
            cp.start()
            fwd.append(cp)

    ccopies = []

    def scale(it, v):
        for cp in flight[v]:
            cp.wait_recv()
        tot = (arb[it, v, 0] + arb[it, v, 1]) + (arb[it, v, 2] + arb[it, v, 3])
        cval = 1.0 / (K * tot)
        cb[v] = jnp.broadcast_to(cval, (8, H))
        if it == ITERS - 1:
            c_out[v, core] = cval
            cp = remote(c_out.at[v, core], c_out.at[v, core], cs.at[v], cr.at[v], mate)
            cp.start()
            ccopies.append(cp)

    lane8 = iota((8, 128), 1)
    sub8 = iota((8, 128), 0)

    def row_pass(it, v):
        def body(i, pack):
            accs = [jnp.zeros((8, 128), F32)] * 8
            for kq in range(0, H // 128, 4):
                ck = [cb[v, :, k * 128:(k + 1) * 128] for k in range(kq, kq + 4)]
                for g in range(8):
                    r0 = pl.multiple_of(i * 64 + g * 8, 8)
                    t = [e[v, pl.ds(r0, 8), (kq + j) * 128:(kq + j + 1) * 128] * ck[j] for j in range(4)]
                    accs[g] = accs[g] + ((t[0] + t[1]) + (t[2] + t[3]))
            for g in range(8):
                rs = jnp.sum(accs[g], axis=1, keepdims=True)
                pack = jnp.where(lane8 == i * 8 + g, rs, pack)
            return pack
        pack = lax.fori_loop(0, 2 * NR // 64, body, jnp.zeros((8, 128), F32))
        rsb[it, v, core] = pack
        cp = remote(rsb.at[it, v, core], rsb.at[it, v, core], rs_.at[it, v], rr.at[it, v], mate)
        cp.start()
        return cp

    def col_pass(it, v, cp):
        cp.wait_recv()
        rtot = rsb[it, v, 0] + rsb[it, v, 1]
        r = 1.0 / (TOTAL * rtot)
        for g in range(2 * NR // 8):
            rb[v, g * 8:(g + 1) * 8, :] = jnp.broadcast_to(r[:, g:g + 1], (8, 128))
        for cc in range(4):
            def body(i, accs):
                accs = list(accs)
                for g in range(8):
                    r0 = pl.multiple_of(i * 64 + g * 8, 8)
                    rg = rb[v, pl.ds(r0, 8), :]
                    for k in range(8):
                        lo = cc * 1024 + k * 128
                        accs[k] = accs[k] + e[v, pl.ds(r0, 8), lo:lo + 128] * rg
                return tuple(accs)
            accs = lax.fori_loop(0, 2 * NR // 64, body, tuple(jnp.zeros((8, 128), F32) for _ in range(8)))
            for k in range(8):
                lo = cc * 1024 + k * 128
                arb[it + 1, v, chip, :, lo:lo + 128] = jnp.sum(accs[k], axis=0, keepdims=True)

    drain = []
    rcopies = []
    for it in range(ITERS - 1):
        cps = []
        for v in range(2):
            scale(it, v)
            cps.append(row_pass(it, v))
        drain += flight[0] + flight[1]
        rcopies += cps
        flight = [None, None]
        for v in range(2):
            col_pass(it, v, cps[v])
            flight[v] = send_cols(it + 1, v)

    def to_row(total, gg, col):
        return total + jnp.where(lane8 == gg * 8 + sub8, col, 0.0)

    def p_pass(v):
        def body(i, total):
            accs = [jnp.zeros((8, 128), F32)] * 8
            for kq in range(0, H // 128, 4):
                for g in range(8):
                    r0 = pl.multiple_of(i * 64 + g * 8, 8)
                    t = [jnp.exp2(sb[v, pl.ds(r0, 8), (kq + j) * 128:(kq + j + 1) * 128] * K10) for j in range(4)]
                    accs[g] = accs[g] + ((t[0] + t[1]) + (t[2] + t[3]))
            for g in range(8):
                total = to_row(total, i * 8 + g, jnp.sum(accs[g], axis=1, keepdims=True))
            return total
        total = lax.fori_loop(0, 2, body, jnp.zeros((8, 128), F32))
        fb[core, 4 + v:5 + v, :] = jnp.sum(total, axis=0, keepdims=True)

    def last_pass(v):
        def body(i, totals):
            tr, tl = totals
            for half in range(2):
                ra = [jnp.zeros((8, 128), F32)] * 4
                la = [jnp.zeros((8, 128), F32)] * 4
                for kq in range(0, H // 128, 4):
                    ck = [cb[v, :, k * 128:(k + 1) * 128] for k in range(kq, kq + 4)]
                    for g in range(4):
                        off = half * 32 + g * 8
                        re = pl.multiple_of(i * NR + off, 8)
                        rb_ = pl.multiple_of(i * NB + off, 8)
                        lanes = [slice((kq + j) * 128, (kq + j + 1) * 128) for j in range(4)]
                        t = [e[v, pl.ds(re, 8), lanes[j]] * ck[j] for j in range(4)]
                        w = [t[j] * sb[1 - v, pl.ds(rb_, 8), lanes[j]] for j in range(4)]
                        ra[g] = ra[g] + ((t[0] + t[1]) + (t[2] + t[3]))
                        la[g] = la[g] + ((w[0] + w[1]) + (w[2] + w[3]))
                for g in range(4):
                    gg = i * 8 + half * 4 + g
                    tr = to_row(tr, gg, jnp.sum(ra[g], axis=1, keepdims=True))
                    tl = to_row(tl, gg, jnp.sum(la[g], axis=1, keepdims=True))
            return tr, tl
        zero = jnp.zeros((8, 128), F32)
        tr, tl = lax.fori_loop(0, 2, body, (zero, zero))
        fb[core, v:v + 1, :] = jnp.sum(tr, axis=0, keepdims=True)
        fb[core, 2 + v:3 + v, :] = jnp.sum(tl, axis=0, keepdims=True)

    fb[core, 6:8, :] = jnp.zeros((2, 128), F32)
    for v in range(2):
        p_pass(v)
    for v in range(2):
        scale(ITERS - 1, v)
        last_pass(v)
    drain += flight[0] + flight[1]
    cp = remote(fb.at[core], fb.at[core], ds_, dr, mate)
    cp.start()
    cp.wait_recv()
    tot = fb[0] + fb[1]
    rinv = 1.0 / tot[0:2]
    pinv = 1.0 / tot[4:6]
    logp = jnp.log(tot[4:6])
    mean = tot[2:4] * rinv * 10.0
    loss = jnp.sum(mean - logp, axis=0, keepdims=True)
    nrm[chip, 0:2, :] = rinv
    nrm[chip, 2:4, :] = pinv
    nrm[chip, 4:5, :] = loss
    nrm[chip, 5:8, :] = jnp.zeros((3, 128), F32)
    ncopies = []
    for p in range(3):
        n = remote(nrm.at[chip], nrm.at[chip], ns.at[p], nr.at[p], peers[p])
        n.start()
        ncopies.append(n)
    cp.wait_send()
    for c in sends + zcopies + drain + rcopies:
        c.wait_send()
    for c in fwd + ccopies + ncopies:
        c.wait()


def sink_call(z1, z2, q1, q2, protos):
    vmem = pl.BlockSpec(memory_space=pltpu.VMEM)
    dma = pltpu.SemaphoreType.DMA
    return pl.pallas_call(
        sink_kernel,
        out_shape=(
            pltpu.VMEM((2, 8 * NB, D), BF16),
            pltpu.VMEM((2, 2, 1, H), F32),
            pltpu.VMEM((4, 8, 128), F32),
        ),
        in_specs=[pl.BlockSpec(memory_space=pltpu.HBM)] * 5,
        out_specs=(vmem, vmem, vmem),
        scratch_shapes=[
            pltpu.VMEM((H, D), BF16),
            pltpu.VMEM((2, 2, NR, D), BF16),
            pltpu.VMEM((2, 2 * NR, H), F32),
            pltpu.VMEM((2, 2 * NB, H), F32),
            pltpu.VMEM((2, 8, H), F32),
            pltpu.VMEM((2, 2 * NR, 128), F32),
            pltpu.VMEM((ITERS, 2, 4, 1, H), F32),
            pltpu.VMEM((ITERS - 1, 2, 2, 8, 128), F32),
            pltpu.VMEM((2, 8, 128), F32),
            dma((2, 3)),
            dma((4,)),
            dma((3, 2)), dma((3, 2)),
            dma((4,)), dma((4,)),
            dma((3, 2)), dma((3, 2)),
            dma((2,)), dma((2,)),
            dma((ITERS, 2, 3)), dma((ITERS, 2, 3)),
            dma((ITERS - 1, 2)), dma((ITERS - 1, 2)),
            dma((3,)), dma((3,)),
            dma, dma,
        ],
        compiler_params=pltpu.CompilerParams(collective_id=0, has_side_effects=True,
                                             vmem_limit_bytes=50 * 1024 * 1024),
        name="sink",
    )(z1, z2, q1, q2, protos)


BK = 256
NSUB = 4
TK = NSUB * BK
FIRST = 2 * TK
COEF = 1.0 / (1024 * 0.1)


def grad_kernel(za, protos, c, nrm, codes1, codes2, dz1, dz2, gp, loss,
                ch, gst, cst, g0, g1, g2, g3, oscr, cc, own, prow, zat, z12, dz, lsem, gsem, csem):
    la = pltpu.make_async_copy(protos.at[pl.ds(0, FIRST)], ch.at[pl.ds(0, FIRST)], lsem.at[0])
    lb = pltpu.make_async_copy(protos.at[pl.ds(FIRST, K - FIRST)], ch.at[pl.ds(FIRST, K - FIRST)], lsem.at[1])
    la.start()
    lb.start()
    me = lax.axis_index("data")
    core = lax.rem(me, 2)
    chip = me // 2
    mine = nrm[chip]
    pick = iota((NB, 128), 1) == iota((NB, 128), 0) + core * NB
    for q in range(4):
        col = jnp.sum(jnp.where(pick, jnp.broadcast_to(mine[q:q + 1], (NB, 128)), 0.0), axis=1, keepdims=True)
        own[q] = jnp.broadcast_to(col, (NB, 128))
        for d in range(4):
            prow[q, d] = jnp.broadcast_to(nrm[d, q:q + 1, :] * COEF, (8, 128))
    tot = jnp.zeros((1, 128), F32)
    for d in range(4):
        tot = tot + nrm[d, 4:5, :]
    loss[...] = jnp.sum(tot, axis=1, keepdims=True) * (-1.0 / 1024)
    for v in range(2):
        z12[v * NB:(v + 1) * NB, :] = za[v, pl.ds(pl.multiple_of(me * NB, NB), NB), :]
        zat[v] = za[v].T
        g3[v] = jnp.zeros((4, BK, 128), BF16)
    oscr[3] = jnp.zeros((2 * NB, BK), BF16)
    dz[...] = jnp.zeros_like(dz)
    codes = (codes1, codes2)
    gs = (g0, g1, g2, g3)

    def block(n):
        return pl.ds(pl.multiple_of(n * BK, BK), BK)

    def gradients(n, k):
        acc = None
        for v in range(2):
            g = jnp.concatenate([gs[k][v, lt] for lt in range(4)], axis=1)
            x = lax.dot_general(g, za[v], NN, preferred_element_type=F32)
            acc = x if acc is None else acc + x
        gst[block(n), :] = acc
        dz[...] += lax.dot_general(oscr[k], ch[block(n), :], NN, preferred_element_type=F32)

    def twice(x):
        return jnp.concatenate([x, x], axis=0)

    def pointwise(n, k):
        ct = ch[block(n), :]
        for rt in range(2):
            s = [lax.dot_general(ct, zat[v, :, rt * 256:(rt + 1) * 256], NN, preferred_element_type=F32)
                 for v in range(2)]
            for b in range(BK // 16):
                rows = slice(b * 16, (b + 1) * 16)
                for l in range(2):
                    lt = rt * 2 + l
                    e = [jnp.exp2(s[v][rows, l * 128:(l + 1) * 128] * K10) for v in range(2)]
                    u = [e[v] * e[v] * cc[v, k * BK + b * 16:k * BK + b * 16 + 16, :] for v in range(2)]
                    for v in range(2):
                        g = e[v] * twice(prow[2 + v, lt]) - u[1 - v] * twice(prow[1 - v, lt])
                        gs[k][v, lt, rows, :] = g.astype(BF16)

    def own_rows(n, k):
        ct = ch[block(n), :]
        s = lax.dot_general(z12[...], ct, NT, preferred_element_type=F32)
        ex = jnp.exp2(s * K10)
        ex = [ex[0:NB], ex[NB:2 * NB]]
        code = []
        for v in range(2):
            q = ex[v] * ex[v] * c[v, :, block(n)] * own[v, :, 0:1]
            cst[v, :, block(n)] = q
            code.append(q)
        for v in range(2):
            g = (ex[v] * own[2 + v, :, 0:1] - code[1 - v]) * COEF
            oscr[k, v * NB:(v + 1) * NB, :] = g.astype(BF16)

    def gcopy(j):
        rows = pl.ds(pl.multiple_of(j * TK, TK), TK)
        return pltpu.make_async_copy(gst.at[rows], gp.at[rows], gsem.at[j])

    def ccopy(v, j):
        cols = pl.ds(pl.multiple_of(j * TK, TK), TK)
        return pltpu.make_async_copy(cst.at[v, :, cols], codes[v].at[:, cols], csem.at[v, j])

    def body(m, carry):
        @pl.when(m >= 1)
        def _():
            ccopy(0, m - 1).start()
            ccopy(1, m - 1).start()

        @pl.when(m >= 2)
        def _():
            gcopy(m - 2).start()

        n = NSUB * m
        for v in range(2):
            crow = c[v, :, pl.ds(pl.multiple_of(m * TK, TK), TK)]
            for b in range(TK // 128):
                cc[v, b * 128:(b + 1) * 128, :] = jnp.broadcast_to(crow[:, b * 128:(b + 1) * 128], (128, 128)).T
        for k in range(NSUB):
            pointwise(n + k, k)
            own_rows(n + k, k)
            if k == 0:
                gradients(jnp.maximum(n - 1, 0), NSUB - 1)
            else:
                gradients(n + k - 1, k - 1)
        return carry

    la.wait()
    lax.fori_loop(0, 2, body, 0)
    lb.wait()
    groups = K // TK
    lax.fori_loop(2, groups, body, 0)
    ccopy(0, groups - 1).start()
    ccopy(1, groups - 1).start()
    gcopy(groups - 2).start()
    gradients(K // BK - 1, NSUB - 1)
    gcopy(groups - 1).start()
    dz1[...] = dz[0:NB]
    dz2[...] = dz[NB:2 * NB]

    def drain(j, carry):
        gcopy(j).wait()
        ccopy(0, j).wait()
        ccopy(1, j).wait()
        return carry

    lax.fori_loop(0, groups, drain, 0)


def grad_call(za, protos, c, nrm):
    vmem = pl.BlockSpec(memory_space=pltpu.VMEM)
    hbm = pl.BlockSpec(memory_space=pl.ANY)
    pin = pl.BlockSpec(memory_space=pltpu.HBM)
    dma = pltpu.SemaphoreType.DMA
    gscr = pltpu.VMEM((2, 4, BK, 128), BF16)
    return pl.pallas_call(
        grad_kernel,
        out_shape=(
            jax.ShapeDtypeStruct((NB, K), F32),
            jax.ShapeDtypeStruct((NB, K), F32),
            jax.ShapeDtypeStruct((NB, D), F32),
            jax.ShapeDtypeStruct((NB, D), F32),
            jax.ShapeDtypeStruct((K, D), F32),
            jax.ShapeDtypeStruct((1, 1), F32),
        ),
        in_specs=[vmem, pin, vmem, vmem],
        out_specs=(hbm, hbm, vmem, vmem, hbm, vmem),
        scratch_shapes=[
            pltpu.VMEM((K, D), BF16),
            pltpu.VMEM((K, D), F32),
            pltpu.VMEM((2, NB, K), F32),
            gscr, gscr, gscr, gscr,
            pltpu.VMEM((NSUB, 2 * NB, BK), BF16),
            pltpu.VMEM((2, TK, 128), F32),
            pltpu.VMEM((4, NB, 128), F32),
            pltpu.VMEM((4, 4, 8, 128), F32),
            pltpu.VMEM((2, D, 8 * NB), BF16),
            pltpu.VMEM((2 * NB, D), BF16),
            pltpu.VMEM((2 * NB, D), F32),
            dma((2,)), dma((K // TK,)), dma((2, K // TK)),
        ],
        compiler_params=pltpu.CompilerParams(vmem_limit_bytes=50 * 1024 * 1024),
        name="grads",
    )(za, protos, c, nrm)


def solution(mesh):
    def local_step(z1, z2, protos, q1, q2):
        z1, z2, q1, q2, protos = (pltpu.with_memory_space_constraint(x, pltpu.HBM) for x in (z1, z2, q1, q2, protos))
        za, c, nrm = sink_call(z1, z2, q1, q2, protos)
        c = c.reshape(2, 1, K)
        codes1, codes2, dz1, dz2, gp, loss = grad_call(za, protos, c, nrm)
        return codes1, codes2, loss.reshape(()), dz1, dz2, gp

    row = P("data", None)
    full = P(None, None)
    return jax.shard_map(
        local_step,
        mesh=mesh,
        in_specs=(row, row, full, row, row),
        out_specs=(row, row, P(), row, row, full),
        check_vma=False,
    )
```

```python
import functools
import math

import jax
import jax.numpy as jnp
from jax import lax
from jax.experimental import pallas as pl
from jax.experimental.pallas import tpu as pltpu
from jax.sharding import PartitionSpec as P

MESH = pl.DeviceIdType.MESH
F32 = jnp.float32
BF16 = jnp.bfloat16
LOG2E = math.log2(math.e)
K20 = 20.0 * LOG2E
K10 = 10.0 * LOG2E
ITERS = 3
NB = 64
NQ = 256
NR = NB + NQ
D = 256
K = 8192
H = K // 2
TOTAL = 8 * NR
T = 1024
NT = (((1,), (1,)), ((), ()))
NN = (((1,), (0,)), ((), ()))


def iota(shape, dim):
    return lax.broadcasted_iota(jnp.int32, shape, dim)


def sink_kernel(z1, z2, q1, q2, protos, za, c_out, nrm,
                ch, xb, e, sb, cb, rb, arb, rsb, fb,
                in_sem, load_sem, zs, zr, xs, xr, fs, fr, cs, cr, as_, ar, rs_, rr, ns, nr, ds_, dr):
    me = lax.axis_index("data")
    core = lax.rem(me, 2)
    chip = me // 2
    px = chip + 1 - 2 * lax.rem(chip, 2)
    py = lax.rem(chip + 2, 4)
    pd = 3 - chip
    peers = [pd * 2 + core, px * 2 + core, py * 2 + core]
    mate = me + 1 - 2 * core
    other = 1 - core

    zrows = pl.ds(pl.multiple_of(me * NB, NB), NB)
    rows_in = []
    for v, (z, q) in enumerate(((z1, q1), (z2, q2))):
        rows_in.append(pltpu.make_async_copy(z, xb.at[core, v, pl.ds(0, NB)], in_sem.at[v, 0]))
        rows_in.append(pltpu.make_async_copy(q, xb.at[core, v, pl.ds(NB, NQ)], in_sem.at[v, 1]))
        rows_in.append(pltpu.make_async_copy(z, za.at[v, zrows], in_sem.at[v, 2]))
    for cp in rows_in:
        cp.start()
    loads = []
    for t in range(4):
        loads.append(pltpu.make_async_copy(
            protos.at[pl.ds(core * H + t * 1024, 1024)], ch.at[pl.ds(t * 1024, 1024)], load_sem.at[t]))
        loads[-1].start()

    bar = pltpu.get_barrier_semaphore()
    for dev in peers + [mate]:
        pl.semaphore_signal(bar, inc=1, device_id=(dev,), device_id_type=MESH)

    def remote(src, dst, ssem, rsem, dev):
        return pltpu.make_async_remote_copy(src_ref=src, dst_ref=dst, send_sem=ssem, recv_sem=rsem,
                                            device_id=(dev,), device_id_type=MESH)

    def score_block(c, first):
        def body(t, carry):
            cols = pl.ds(pl.multiple_of(t * T, T), T)
            ct = ch[cols, :]
            for v in range(2):
                s = lax.dot_general(xb[c, v], ct, NT, preferred_element_type=F32)
                ex = jnp.exp2(s * K20)
                e[v, pl.ds(pl.multiple_of(c * NR, NB), NR), cols] = ex
                sb[v, pl.ds(pl.multiple_of(c * NB, NB), NB), cols] = s[0:NB]
                col = jnp.sum(ex, axis=0, keepdims=True)
                if first:
                    arb[0, v, chip, :, cols] = col
                else:
                    arb[0, v, chip, :, cols] = arb[0, v, chip, :, cols] + col
            return carry
        return body

    for cp in rows_in:
        cp.wait()
    loads[0].wait()
    score_block(core, True)(0, 0)
    pl.semaphore_wait(bar, 4)
    sends = []
    for v in range(2):
        cp = remote(xb.at[core, v], xb.at[core, v], xs.at[v], xr.at[v], mate)
        cp.start()
        sends.append(cp)
        cp = remote(za.at[v, zrows], za.at[v, zrows], xs.at[2 + v], xr.at[2 + v], mate)
        cp.start()
        sends.append(cp)
    zcopies = []
    for p in range(3):
        for v in range(2):
            cp = remote(za.at[v, zrows], za.at[v, zrows], zs.at[p, v], zr.at[p, v], peers[p])
            cp.start()
            zcopies.append(cp)
    for t in range(1, 4):
        loads[t].wait()
    lax.fori_loop(1, H // T, score_block(core, True), 0)

    for cp in sends:
        cp.wait_recv()
    lax.fori_loop(0, H // T, score_block(other, False), 0)

    def send_cols(it, v):
        out = []
        for p in range(3):
            cp = remote(arb.at[it, v, chip], arb.at[it, v, chip], as_.at[it, v, p], ar.at[it, v, p], peers[p])
            cp.start()
            out.append(cp)
        return out

    flight = [send_cols(0, v) for v in range(2)]

    for cp in zcopies:
        cp.wait_recv()
    fwd = []
    for p in range(3):
        rows = pl.ds(pl.multiple_of(peers[p] * NB, NB), NB)
        for v in range(2):
            cp = remote(za.at[v, rows], za.at[v, rows], fs.at[p, v], fr.at[p, v], mate)
            cp.start()
            fwd.append(cp)

    ccopies = []

    def scale(it, v):
        for cp in flight[v]:
            cp.wait_recv()
        tot = (arb[it, v, 0] + arb[it, v, 1]) + (arb[it, v, 2] + arb[it, v, 3])
        cval = 1.0 / (K * tot)
        cb[v] = jnp.broadcast_to(cval, (8, H))
        if it == ITERS - 1:
            c_out[v, core] = cval
            cp = remote(c_out.at[v, core], c_out.at[v, core], cs.at[v], cr.at[v], mate)
            cp.start()
            ccopies.append(cp)

    lane8 = iota((8, 128), 1)
    sub8 = iota((8, 128), 0)

    def row_pass(it, v):
        def body(i, pack):
            accs = [jnp.zeros((8, 128), F32)] * 16
            for kq in range(0, H // 128, 4):
                ck = [cb[v, :, k * 128:(k + 1) * 128] for k in range(kq, kq + 4)]
                for g in range(16):
                    r0 = pl.multiple_of(i * 128 + g * 8, 8)
                    t = [e[v, pl.ds(r0, 8), (kq + j) * 128:(kq + j + 1) * 128] * ck[j] for j in range(4)]
                    accs[g] = accs[g] + ((t[0] + t[1]) + (t[2] + t[3]))
            for g in range(16):
                rs = jnp.sum(accs[g], axis=1, keepdims=True)
                pack = jnp.where(lane8 == i * 16 + g, rs, pack)
            return pack
        pack = lax.fori_loop(0, 2 * NR // 128, body, jnp.zeros((8, 128), F32))
        rsb[it, v, core] = pack
        cp = remote(rsb.at[it, v, core], rsb.at[it, v, core], rs_.at[it, v], rr.at[it, v], mate)
        cp.start()
        return cp

    def col_pass(it, v, cp):
        cp.wait_recv()
        rtot = rsb[it, v, 0] + rsb[it, v, 1]
        r = 1.0 / (TOTAL * rtot)
        for g in range(2 * NR // 8):
            rb[v, g * 8:(g + 1) * 8, :] = jnp.broadcast_to(r[:, g:g + 1], (8, 128))
        for cc in range(4):
            def body(i, accs):
                accs = list(accs)
                for g in range(16):
                    r0 = pl.multiple_of(i * 128 + g * 8, 8)
                    rg = rb[v, pl.ds(r0, 8), :]
                    for k in range(8):
                        lo = cc * 1024 + k * 128
                        accs[k] = accs[k] + e[v, pl.ds(r0, 8), lo:lo + 128] * rg
                return tuple(accs)
            accs = lax.fori_loop(0, 2 * NR // 128, body, tuple(jnp.zeros((8, 128), F32) for _ in range(8)))
            for k in range(8):
                lo = cc * 1024 + k * 128
                arb[it + 1, v, chip, :, lo:lo + 128] = jnp.sum(accs[k], axis=0, keepdims=True)

    drain = []
    rcopies = []
    for it in range(ITERS - 1):
        cps = []
        for v in range(2):
            scale(it, v)
            cps.append(row_pass(it, v))
        drain += flight[0] + flight[1]
        rcopies += cps
        flight = [None, None]
        for v in range(2):
            col_pass(it, v, cps[v])
            flight[v] = send_cols(it + 1, v)

    def to_row(total, gg, col):
        return total + jnp.where(lane8 == gg * 8 + sub8, col, 0.0)

    def p_pass(v):
        def body(i, total):
            accs = [jnp.zeros((8, 128), F32)] * 8
            for kq in range(0, H // 128, 4):
                for g in range(8):
                    r0 = pl.multiple_of(i * 64 + g * 8, 8)
                    t = [jnp.exp2(sb[v, pl.ds(r0, 8), (kq + j) * 128:(kq + j + 1) * 128] * K10) for j in range(4)]
                    accs[g] = accs[g] + ((t[0] + t[1]) + (t[2] + t[3]))
            for g in range(8):
                total = to_row(total, i * 8 + g, jnp.sum(accs[g], axis=1, keepdims=True))
            return total
        total = lax.fori_loop(0, 2, body, jnp.zeros((8, 128), F32))
        fb[core, 4 + v:5 + v, :] = jnp.sum(total, axis=0, keepdims=True)

    def last_pass(v):
        def body(i, totals):
            tr, tl = totals
            for half in range(2):
                ra = [jnp.zeros((8, 128), F32)] * 4
                la = [jnp.zeros((8, 128), F32)] * 4
                for kq in range(0, H // 128, 4):
                    ck = [cb[v, :, k * 128:(k + 1) * 128] for k in range(kq, kq + 4)]
                    for g in range(4):
                        off = half * 32 + g * 8
                        re = pl.multiple_of(i * NR + off, 8)
                        rb_ = pl.multiple_of(i * NB + off, 8)
                        lanes = [slice((kq + j) * 128, (kq + j + 1) * 128) for j in range(4)]
                        t = [e[v, pl.ds(re, 8), lanes[j]] * ck[j] for j in range(4)]
                        w = [t[j] * sb[1 - v, pl.ds(rb_, 8), lanes[j]] for j in range(4)]
                        ra[g] = ra[g] + ((t[0] + t[1]) + (t[2] + t[3]))
                        la[g] = la[g] + ((w[0] + w[1]) + (w[2] + w[3]))
                for g in range(4):
                    gg = i * 8 + half * 4 + g
                    tr = to_row(tr, gg, jnp.sum(ra[g], axis=1, keepdims=True))
                    tl = to_row(tl, gg, jnp.sum(la[g], axis=1, keepdims=True))
            return tr, tl
        zero = jnp.zeros((8, 128), F32)
        tr, tl = lax.fori_loop(0, 2, body, (zero, zero))
        fb[core, v:v + 1, :] = jnp.sum(tr, axis=0, keepdims=True)
        fb[core, 2 + v:3 + v, :] = jnp.sum(tl, axis=0, keepdims=True)

    fb[core, 6:8, :] = jnp.zeros((2, 128), F32)
    for v in range(2):
        p_pass(v)
    for v in range(2):
        scale(ITERS - 1, v)
        last_pass(v)
    drain += flight[0] + flight[1]
    cp = remote(fb.at[core], fb.at[core], ds_, dr, mate)
    cp.start()
    cp.wait_recv()
    tot = fb[0] + fb[1]
    rinv = 1.0 / tot[0:2]
    pinv = 1.0 / tot[4:6]
    logp = jnp.log(tot[4:6])
    mean = tot[2:4] * rinv * 10.0
    loss = jnp.sum(mean - logp, axis=0, keepdims=True)
    nrm[chip, 0:2, :] = rinv
    nrm[chip, 2:4, :] = pinv
    nrm[chip, 4:5, :] = loss
    nrm[chip, 5:8, :] = jnp.zeros((3, 128), F32)
    ncopies = []
    for p in range(3):
        n = remote(nrm.at[chip], nrm.at[chip], ns.at[p], nr.at[p], peers[p])
        n.start()
        ncopies.append(n)
    cp.wait_send()
    for c in sends + zcopies + drain + rcopies:
        c.wait_send()
    for c in fwd + ccopies + ncopies:
        c.wait()


def sink_call(z1, z2, q1, q2, protos):
    vmem = pl.BlockSpec(memory_space=pltpu.VMEM)
    dma = pltpu.SemaphoreType.DMA
    return pl.pallas_call(
        sink_kernel,
        out_shape=(
            pltpu.VMEM((2, 8 * NB, D), BF16),
            pltpu.VMEM((2, 2, 1, H), F32),
            pltpu.VMEM((4, 8, 128), F32),
        ),
        in_specs=[pl.BlockSpec(memory_space=pltpu.HBM)] * 5,
        out_specs=(vmem, vmem, vmem),
        scratch_shapes=[
            pltpu.VMEM((H, D), BF16),
            pltpu.VMEM((2, 2, NR, D), BF16),
            pltpu.VMEM((2, 2 * NR, H), F32),
            pltpu.VMEM((2, 2 * NB, H), F32),
            pltpu.VMEM((2, 8, H), F32),
            pltpu.VMEM((2, 2 * NR, 128), F32),
            pltpu.VMEM((ITERS, 2, 4, 1, H), F32),
            pltpu.VMEM((ITERS - 1, 2, 2, 8, 128), F32),
            pltpu.VMEM((2, 8, 128), F32),
            dma((2, 3)),
            dma((4,)),
            dma((3, 2)), dma((3, 2)),
            dma((4,)), dma((4,)),
            dma((3, 2)), dma((3, 2)),
            dma((2,)), dma((2,)),
            dma((ITERS, 2, 3)), dma((ITERS, 2, 3)),
            dma((ITERS - 1, 2)), dma((ITERS - 1, 2)),
            dma((3,)), dma((3,)),
            dma, dma,
        ],
        compiler_params=pltpu.CompilerParams(collective_id=0, has_side_effects=True,
                                             vmem_limit_bytes=50 * 1024 * 1024),
        name="sink",
    )(z1, z2, q1, q2, protos)


BK = 256
NSUB = 4
TK = NSUB * BK
FIRST = 2 * TK
COEF = 1.0 / (1024 * 0.1)


def grad_kernel(za, protos, c, nrm, codes1, codes2, dz1, dz2, gp, loss,
                ch, gst, cst, g0, g1, g2, g3, oscr, cc, own, prow, zat, z12, dz, lsem, gsem, csem):
    la = pltpu.make_async_copy(protos.at[pl.ds(0, FIRST)], ch.at[pl.ds(0, FIRST)], lsem.at[0])
    lb = pltpu.make_async_copy(protos.at[pl.ds(FIRST, K - FIRST)], ch.at[pl.ds(FIRST, K - FIRST)], lsem.at[1])
    la.start()
    lb.start()
    me = lax.axis_index("data")
    core = lax.rem(me, 2)
    chip = me // 2
    mine = nrm[chip]
    pick = iota((NB, 128), 1) == iota((NB, 128), 0) + core * NB
    for q in range(4):
        col = jnp.sum(jnp.where(pick, jnp.broadcast_to(mine[q:q + 1], (NB, 128)), 0.0), axis=1, keepdims=True)
        own[q] = jnp.broadcast_to(col, (NB, 128))
        for d in range(4):
            prow[q, d] = jnp.broadcast_to(nrm[d, q:q + 1, :] * COEF, (8, 128))
    tot = jnp.zeros((1, 128), F32)
    for d in range(4):
        tot = tot + nrm[d, 4:5, :]
    loss[...] = jnp.sum(tot, axis=1, keepdims=True) * (-1.0 / 1024)
    for v in range(2):
        z12[v * NB:(v + 1) * NB, :] = za[v, pl.ds(pl.multiple_of(me * NB, NB), NB), :]
        zat[v] = za[v].T
        g3[v] = jnp.zeros((4, BK, 128), BF16)
    oscr[3] = jnp.zeros((2 * NB, BK), BF16)
    dz[...] = jnp.zeros_like(dz)
    codes = (codes1, codes2)
    gs = (g0, g1, g2, g3)

    def block(n):
        return pl.ds(pl.multiple_of(n * BK, BK), BK)

    def gradients(n, k):
        acc = None
        for v in range(2):
            g = jnp.concatenate([gs[k][v, lt] for lt in range(4)], axis=1)
            x = lax.dot_general(g, za[v], NN, preferred_element_type=F32)
            acc = x if acc is None else acc + x
        gst[block(n), :] = acc
        dz[...] += lax.dot_general(oscr[k], ch[block(n), :], NN, preferred_element_type=F32)

    def twice(x):
        return jnp.concatenate([x, x], axis=0)

    def pointwise(n, k):
        ct = ch[block(n), :]
        for rt in range(2):
            s = [lax.dot_general(ct, zat[v, :, rt * 256:(rt + 1) * 256], NN, preferred_element_type=F32)
                 for v in range(2)]
            for b in range(BK // 16):
                rows = slice(b * 16, (b + 1) * 16)
                for l in range(2):
                    lt = rt * 2 + l
                    e = [jnp.exp2(s[v][rows, l * 128:(l + 1) * 128] * K10) for v in range(2)]
                    u = [e[v] * e[v] * cc[v, k * BK + b * 16:k * BK + b * 16 + 16, :] for v in range(2)]
                    for v in range(2):
                        g = e[v] * twice(prow[2 + v, lt]) - u[1 - v] * twice(prow[1 - v, lt])
                        gs[k][v, lt, rows, :] = g.astype(BF16)

    def own_rows(n, k):
        ct = ch[block(n), :]
        s = lax.dot_general(z12[...], ct, NT, preferred_element_type=F32)
        ex = jnp.exp2(s * K10)
        ex = [ex[0:NB], ex[NB:2 * NB]]
        code = []
        for v in range(2):
            q = ex[v] * ex[v] * c[v, :, block(n)] * own[v, :, 0:1]
            cst[v, :, block(n)] = q
            code.append(q)
        for v in range(2):
            g = (ex[v] * own[2 + v, :, 0:1] - code[1 - v]) * COEF
            oscr[k, v * NB:(v + 1) * NB, :] = g.astype(BF16)

    def gcopy(j):
        rows = pl.ds(pl.multiple_of(j * TK, TK), TK)
        return pltpu.make_async_copy(gst.at[rows], gp.at[rows], gsem.at[j])

    def ccopy(v, j):
        cols = pl.ds(pl.multiple_of(j * TK, TK), TK)
        return pltpu.make_async_copy(cst.at[v, :, cols], codes[v].at[:, cols], csem.at[v, j])

    def body(m, carry):
        @pl.when(m >= 1)
        def _():
            ccopy(0, m - 1).start()
            ccopy(1, m - 1).start()

        @pl.when(m >= 2)
        def _():
            gcopy(m - 2).start()

        n = NSUB * m
        for v in range(2):
            crow = c[v, :, pl.ds(pl.multiple_of(m * TK, TK), TK)]
            for b in range(TK // 128):
                cc[v, b * 128:(b + 1) * 128, :] = jnp.broadcast_to(crow[:, b * 128:(b + 1) * 128], (128, 128)).T
        for k in range(NSUB):
            pointwise(n + k, k)
            own_rows(n + k, k)
            if k == 0:
                gradients(jnp.maximum(n - 1, 0), NSUB - 1)
            else:
                gradients(n + k - 1, k - 1)
        return carry

    la.wait()
    lax.fori_loop(0, 2, body, 0)
    lb.wait()
    groups = K // TK
    lax.fori_loop(2, groups, body, 0)
    ccopy(0, groups - 1).start()
    ccopy(1, groups - 1).start()
    gcopy(groups - 2).start()
    gradients(K // BK - 1, NSUB - 1)
    gcopy(groups - 1).start()
    dz1[...] = dz[0:NB]
    dz2[...] = dz[NB:2 * NB]

    def drain(j, carry):
        gcopy(j).wait()
        ccopy(0, j).wait()
        ccopy(1, j).wait()
        return carry

    lax.fori_loop(0, groups, drain, 0)


def grad_call(za, protos, c, nrm):
    vmem = pl.BlockSpec(memory_space=pltpu.VMEM)
    hbm = pl.BlockSpec(memory_space=pl.ANY)
    pin = pl.BlockSpec(memory_space=pltpu.HBM)
    dma = pltpu.SemaphoreType.DMA
    gscr = pltpu.VMEM((2, 4, BK, 128), BF16)
    return pl.pallas_call(
        grad_kernel,
        out_shape=(
            jax.ShapeDtypeStruct((NB, K), F32),
            jax.ShapeDtypeStruct((NB, K), F32),
            jax.ShapeDtypeStruct((NB, D), F32),
            jax.ShapeDtypeStruct((NB, D), F32),
            jax.ShapeDtypeStruct((K, D), F32),
            jax.ShapeDtypeStruct((1, 1), F32),
        ),
        in_specs=[vmem, pin, vmem, vmem],
        out_specs=(hbm, hbm, vmem, vmem, hbm, vmem),
        scratch_shapes=[
            pltpu.VMEM((K, D), BF16),
            pltpu.VMEM((K, D), F32),
            pltpu.VMEM((2, NB, K), F32),
            gscr, gscr, gscr, gscr,
            pltpu.VMEM((NSUB, 2 * NB, BK), BF16),
            pltpu.VMEM((2, TK, 128), F32),
            pltpu.VMEM((4, NB, 128), F32),
            pltpu.VMEM((4, 4, 8, 128), F32),
            pltpu.VMEM((2, D, 8 * NB), BF16),
            pltpu.VMEM((2 * NB, D), BF16),
            pltpu.VMEM((2 * NB, D), F32),
            dma((2,)), dma((K // TK,)), dma((2, K // TK)),
        ],
        compiler_params=pltpu.CompilerParams(vmem_limit_bytes=50 * 1024 * 1024),
        name="grads",
    )(za, protos, c, nrm)


def solution(mesh):
    def local_step(z1, z2, protos, q1, q2):
        z1, z2, q1, q2, protos = (pltpu.with_memory_space_constraint(x, pltpu.HBM) for x in (z1, z2, q1, q2, protos))
        za, c, nrm = sink_call(z1, z2, q1, q2, protos)
        c = c.reshape(2, 1, K)
        codes1, codes2, dz1, dz2, gp, loss = grad_call(za, protos, c, nrm)
        return codes1, codes2, loss.reshape(()), dz1, dz2, gp

    row = P("data", None)
    full = P(None, None)
    return jax.shard_map(
        local_step,
        mesh=mesh,
        in_specs=(row, row, full, row, row),
        out_specs=(row, row, P(), row, row, full),
        check_vma=False,
    )
```
